32 devices in a mesh: plant: 2 (over x), section: 16 (over z, y, core).
Axes of the slice: x: 2, y: 2, z: 4, core: 2. Of those that a mesh axis runs over, the one named last changes fastest.
Arguments:
- dynamics_operator: bfloat16 [1024, 512], P('plant'), parts along dimension 0
- control_gain_array: bfloat16 [1024, 256], P('plant'), parts along dimension 0
- kkt_inverse: bfloat16 [1536, 768], P('plant'), parts along dimension 0
- lin_state: float32 [1024, 4096], P(('plant', 'section')), parts along dimension 0, may hold values from -6 to 6
- lin_input: float32 [512, 4096], P(('plant', 'section')), parts along dimension 0, may hold values from -6 to 6
- block_start: int32 [2], P('plant'), parts along dimension 0, may hold values from 0 to 15
- period: int32 [2], P('plant'), parts along dimension 0, may hold values from 2048 to 4096
Outputs:
- state_traj: float32 [1024, 4096], P('plant', 'section'), parts along dimension 0
- input_traj: float32 [512, 4096], P('plant', 'section'), parts along dimension 0
- consensus: float32 [1024, 4096], P('plant', 'section'), parts along dimension 0
- residual_norms: float32 [4], P('plant'), parts along dimension 0
The draws below stay inside these ranges and needn't reach their ends.
There are 2 independent parts, one for each index of `plant`. The reference program is written for one: setup_inputs(seed, part) draws one part's arguments, and reference() takes and returns one part's arrays. A program takes and returns all parts, laid end to end along the dimension named above; each array names one. Nothing has to cross between parts.
Inputs may be any that keep to these rules, and one draw needn't show every extreme that they name: Device d of the section axis holds the block of logical sections starting at 256 * ((d - block_start) mod the axis's size).
All inputs are finite; a program needn't handle non-finite values.
Results may differ from the reference program's by a relative error of at most 0.0045.
Values sent between devices are 32-bit elements; how exact they have to be, the bound alone decides.
A program may use at most 64 MiB of HBM per device.

```python
import jax
import jax.numpy as jnp
from jax import lax

STATE = 512
INPUT = 256
ITERS = 4
SECTIONS = 4096
N_SECTION = 16


RHO = 1.0


def plant_system(key):
    key_a = jax.random.fold_in(key, 11)
    key_b = jax.random.fold_in(key, 23)
    key_state = jax.random.fold_in(key, 37)
    key_input = jax.random.fold_in(key, 41)
    dynamics_operator = (jax.random.normal(key_a, (STATE, STATE), jnp.float32) / jnp.sqrt(jnp.float32(STATE))).astype(jnp.bfloat16)
    control_gain_array = (jax.random.normal(key_b, (STATE, INPUT), jnp.float32) / jnp.sqrt(jnp.float32(INPUT))).astype(jnp.bfloat16)
    low_end, high_end = (0.5, 5.0)
    state_weight = jnp.exp(jax.random.uniform(key_state, (STATE,), jnp.float32, jnp.log(low_end), jnp.log(high_end)))
    input_weight = jnp.exp(jax.random.uniform(key_input, (INPUT,), jnp.float32, jnp.log(0.1), jnp.log(1.0)))
    merged_pieces = jnp.concatenate([dynamics_operator, control_gain_array], axis=1).astype(jnp.float32)
    hessian = RHO * jnp.dot(merged_pieces.T, merged_pieces, precision=lax.Precision.HIGHEST)
    hessian = hessian + jnp.diag(jnp.concatenate([state_weight + RHO, input_weight]))
    inverse = jnp.linalg.inv(hessian)
    return (dynamics_operator, control_gain_array, inverse.astype(jnp.bfloat16))


def draw_dynamics_operator(key, part):
    return plant_system(key)[0]


def draw_control_gain_array(key, part):
    return plant_system(key)[1]


def draw_kkt_inverse(key, part):
    return plant_system(key)[2]


def levels(stream_key, shape, cuts, smallest, largest):
    def one(position, shards_of):
        steps = jax.random.uniform(jax.random.fold_in(jax.random.fold_in(stream_key, 6), position), (shards_of,), jnp.float32, smallest / len(cuts), largest / len(cuts))
        return jnp.repeat(jnp.exp(steps), shape[position] // shards_of).reshape((-1,) + (1,) * (len(shape) - position - 1))

    loudness = one(*cuts[0])
    for cut in cuts[1:]:
        loudness = loudness * one(*cut)
    return loudness


def noise(rng, shape, scale, most, split=(), kind=jnp.bfloat16):
    factor_of = levels(rng, shape, split, -0.22, 0.18) if split else 1.0
    entries = jax.random.normal(rng, shape, jnp.float32) * scale * factor_of
    return jnp.minimum(jnp.maximum(entries, -most), most).astype(kind)


def setup_inputs(seed: int = 0, part: int = 0) -> dict:
    key_of = jax.random.split(jax.random.key(seed), 8)
    own_keys = jax.random.split(jax.random.fold_in(key_of[7], part), 8)
    return {
        "dynamics_operator": draw_dynamics_operator(jax.random.fold_in(jax.random.fold_in(key_of[7], part), 71), part),
        "control_gain_array": draw_control_gain_array(jax.random.fold_in(jax.random.fold_in(key_of[7], part), 71), part),
        "kkt_inverse": draw_kkt_inverse(jax.random.fold_in(jax.random.fold_in(key_of[7], part), 71), part),
        "lin_state": noise(own_keys[3], (STATE, SECTIONS), 1.0, 6.0, ((0, 16),), jnp.float32),
        "lin_input": noise(own_keys[4], (INPUT, SECTIONS), 1.0, 6.0, ((0, 16),), jnp.float32),
        "block_start": jax.random.randint(own_keys[5], (1,), 0, N_SECTION).astype(jnp.int32),
        "period": jax.random.randint(own_keys[6], (1,), SECTIONS // 2, SECTIONS + 1).astype(jnp.int32),
    }


RHO = 1.0

def adjoint(dynamics_operator, control_gain_array, target):
    rounded = target.astype(jnp.bfloat16)
    contract = (((0,), (0,)), ((), ()))
    upper_part = lax.dot_general(dynamics_operator.astype(jnp.float32), rounded.astype(jnp.float32), contract, preferred_element_type=jnp.float32)
    lower_part = lax.dot_general(control_gain_array.astype(jnp.float32), rounded.astype(jnp.float32), contract, preferred_element_type=jnp.float32)
    return jnp.concatenate([upper_part, lower_part], axis=0)

def estimate_condition(dynamics_operator, control_gain_array, merged_pieces, condition_lines):
    rounded = merged_pieces.astype(jnp.bfloat16)
    return jnp.dot(dynamics_operator.astype(jnp.float32), rounded[:condition_lines].astype(jnp.float32), preferred_element_type=jnp.float32) + jnp.dot(control_gain_array.astype(jnp.float32), rounded[condition_lines:].astype(jnp.float32), preferred_element_type=jnp.float32)

def reference(dynamics_operator, control_gain_array, kkt_inverse, lin_state, lin_input, block_start, period):
    condition_lines = dynamics_operator.shape[0]
    block_width = lin_state.shape[1] // N_SECTION
    offset = (block_start[0] * block_width).astype(jnp.int32)
    neg_cost = -jnp.concatenate([jnp.roll(lin_state, -offset, 1), jnp.roll(lin_input, -offset, 1)], axis=0)
    section_total = neg_cost.shape[1]
    section_ids = jnp.arange(section_total, dtype=jnp.int32)
    working_segment = (section_ids < period[0])[None, :]
    is_first = (section_ids == 0)[None, :]
    stop_index = (period[0] - 1).astype(jnp.int32)
    is_last = (section_ids == stop_index)[None, :]
    zero_block = jnp.zeros((condition_lines, section_total), jnp.float32)
    input_zero = jnp.zeros((neg_cost.shape[0] - condition_lines, section_total), jnp.float32)
    consensus = zero_block
    dual_state = zero_block
    multiplier_link = zero_block
    ahead_z = zero_block
    feasibility_gap_total = jnp.float32(0.0)
    dual_sum = jnp.float32(0.0)
    merged_pieces = jnp.zeros_like(neg_cost)
    for iteration in range(ITERS):
        right_side = neg_cost + RHO * jnp.concatenate([consensus - dual_state, input_zero], axis=0) + RHO * adjoint(dynamics_operator, control_gain_array, ahead_z - multiplier_link)
        product = jnp.dot(kkt_inverse.astype(jnp.float32), right_side.astype(jnp.bfloat16).astype(jnp.float32), preferred_element_type=jnp.float32)
        merged_pieces = jnp.where(working_segment, product, 0.0)
        expected_condition = estimate_condition(dynamics_operator, control_gain_array, merged_pieces, condition_lines)
        own_sum = merged_pieces[:condition_lines] + dual_state
        passed_quantity = expected_condition + multiplier_link
        previous = jnp.roll(passed_quantity, 1, axis=1)
        closing_carried = lax.dynamic_slice_in_dim(passed_quantity, stop_index, 1, 1)
        previous = jnp.where(is_first, closing_carried, previous)
        newest_agreement = jnp.where(working_segment, 0.5 * (own_sum + previous), 0.0)
        onward_refreshed = jnp.where(is_last, newest_agreement[:, 0:1], jnp.roll(newest_agreement, -1, axis=1))
        change_z = newest_agreement - consensus
        dual_state = jnp.where(working_segment, dual_state + merged_pieces[:condition_lines] - newest_agreement, 0.0)
        multiplier_link = jnp.where(working_segment, multiplier_link + expected_condition - onward_refreshed, 0.0)
        feasibility_gap_total = jnp.sum(jnp.where(working_segment, (merged_pieces[:condition_lines] - newest_agreement) ** 2 + (expected_condition - onward_refreshed) ** 2, 0.0))
        dual_sum = RHO * RHO * jnp.sum(change_z * change_z)
        consensus = newest_agreement
        ahead_z = onward_refreshed
    state_traj = jnp.roll(merged_pieces[:condition_lines], offset, 1)
    input_traj = jnp.roll(merged_pieces[condition_lines:], offset, 1)
    consensus_out = jnp.roll(consensus, offset, 1)
    residual_norms = jnp.stack([jnp.sqrt(feasibility_gap_total), jnp.sqrt(dual_sum)]).astype(jnp.float32)
    return (state_traj, input_traj, consensus_out, residual_norms)
```

```python
import functools

import jax
import jax.numpy as jnp
from jax import lax
from jax.experimental import pallas as pl
from jax.experimental.pallas import tpu as pltpu
from jax.sharding import PartitionSpec as P

ITERS = 4
RHO = 1.0
LANES = 128
SUB = 8
CHUNK = 512
TILE = 256
ROWS = 16
NT = (((1,), (1,)), ((), ()))


def dot(a, b):
    return jnp.dot(a, b, preferred_element_type=jnp.float32)


def scaled(value):
    return value if RHO == 1.0 else RHO * value


def partner(me, k, n, sign):
    if n & (n - 1):
        return lax.rem(me + sign * k + n, n)
    other = me
    for bit in range(n.bit_length()):
        if (k >> bit) & 1:
            other = other + (1 - 2 * ((me // (1 << bit)) % 2)) * (1 << bit)
    return other


def kernel(
    n, width,
    a_hbm, b_hbm, k_hbm, cs_hbm, ci_hbm, start_hbm, period_hbm,
    x_out, u_out, z_out, norm_out,
    ab, abt, kkt, kt, cs, ci, recv_s, recv_i, cpad, hsend, recv_h, hrow,
    negc, rhs, w, wb, pred, link, zn, y, v, c, z, g, xo, uo, zo, part, recv_p,
    start_ref, period_ref,
    load_sem, send_sem, recv_sem, out_sem,
):
    me = lax.axis_index("section")
    nx = a_hbm.shape[0]
    nu = b_hbm.shape[1]
    nw = nx + nu
    rs, ri = cs.shape[0], ci.shape[0]
    rows = width + 2 * SUB
    half = LANES // 2

    def cols(i):
        return pl.ds(pl.multiple_of(i * width, LANES), width)

    loads = [
        pltpu.make_async_copy(cs_hbm, cs, load_sem.at[0]),
        pltpu.make_async_copy(ci_hbm, ci, load_sem.at[1]),
        pltpu.make_async_copy(start_hbm, start_ref, load_sem.at[2]),
        pltpu.make_async_copy(period_hbm, period_ref, load_sem.at[3]),
        pltpu.make_async_copy(a_hbm, ab.at[:, pl.ds(0, nx)], load_sem.at[4]),
        pltpu.make_async_copy(b_hbm, ab.at[:, pl.ds(nx, nu)], load_sem.at[5]),
        pltpu.make_async_copy(k_hbm, kkt, load_sem.at[6]),
        pltpu.make_async_copy(cs_hbm.at[:, cols(me)], recv_s.at[me], load_sem.at[7]),
        pltpu.make_async_copy(ci_hbm.at[:, cols(me)], recv_i.at[me], load_sem.at[8]),
    ]
    barrier = pltpu.get_barrier_semaphore()
    for k in range(1, n):
        pl.semaphore_signal(barrier, inc=1, device_id={"section": partner(me, k, n, 1)})
    for copy in loads:
        copy.start()

    def copies(kind, k, incoming=False):
        to = partner(me, k, n, 1)
        if kind == 0:
            src, dst = part, recv_p
        elif kind == 1:
            src, dst = hsend.at[to], recv_h
        elif kind == 2:
            src, dst = cs.at[:, cols(to)], recv_s
        else:
            src, dst = ci.at[:, cols(to)], recv_i
        slot = partner(me, k, n, -1) if incoming else me
        return pltpu.make_async_remote_copy(
            src_ref=src, dst_ref=dst.at[slot], send_sem=send_sem.at[kind, k],
            recv_sem=recv_sem.at[kind, slot], device_id={"section": to},
        )

    order = list(range(n // 2, n)) + list(range(n // 2 - 1, 0, -1))

    for copy in loads[:4]:
        copy.wait()
    start = start_ref[0]
    period = period_ref[0]

    row = lax.broadcasted_iota(jnp.int32, (n * SUB, 1), 0)
    late = row >= n * ITERS
    row = jnp.where(late, row - n * ITERS, row)
    block = row // ITERS - start
    block = jnp.where(block < 0, block + n, block)
    base = block * width
    item = row % ITERS
    ahead = base + jnp.minimum(period - base, width) + item
    ahead = jnp.where(ahead >= period, ahead - period, ahead)
    behind = base + item - ITERS
    behind = jnp.where(behind < 0, behind + period, behind)
    place = jnp.where(late, behind, ahead) + start * width
    place = jnp.where(place >= n * width, place - n * width, place)

    cpad[...] = jnp.zeros_like(cpad)

    def pick(j, total):
        at = pl.ds(pl.multiple_of(j * CHUNK, CHUNK), CHUNK)
        cpad[pl.ds(0, rs), :] = cs[:, at]
        cpad[pl.ds(rs, ri), :] = ci[:, at]
        column = lax.broadcasted_iota(jnp.int32, (n * SUB, CHUNK), 1) + j * CHUNK
        onehot = jnp.where(column == place, 1.0, 0.0).astype(jnp.bfloat16)
        rest = cpad[...]
        for _ in range(3):
            piece = rest.astype(jnp.bfloat16)
            rest = rest - piece.astype(jnp.float32)
            total = total + lax.dot_general(onehot, piece, NT, preferred_element_type=jnp.float32)
        return total

    picked = lax.fori_loop(
        0, cs.shape[1] // CHUNK, pick, jnp.zeros((n * SUB, LANES), jnp.float32)
    )
    packed = picked[:n * ITERS] + pltpu.roll(picked[n * ITERS:], half, 1)
    hsend[...] = packed.reshape(n, ITERS, LANES)
    recv_h[me] = hsend[me]

    pl.semaphore_wait(barrier, n - 1)
    for k in order:
        copies(1, k).start()
    for k in order:
        copies(2, k).start()
        copies(3, k).start()

    for copy in loads[4:7]:
        copy.wait()
    abt[...] = ab[...].T
    kt[...] = kkt[...].T
    link[pl.ds(0, SUB), :] = jnp.zeros((SUB, nx), jnp.float32)
    zn[pl.ds(rows, SUB), :] = jnp.zeros((SUB, nx), jnp.float32)

    mine = me - start
    mine = jnp.where(mine < 0, mine + n, mine)
    base = mine * width
    finish = jnp.minimum(period - base, width)

    for k in order:
        copies(1, k, True).wait_recv()

    lane = lax.broadcasted_iota(jnp.int32, (ITERS, LANES), 1)
    phase = (finish + 2 * width) % SUB
    for r, top in ((rs, 0), (ri, nx)):
        off = 0 if top == 0 else rs
        per = LANES // r
        for t in range(0, n * r, LANES):
            fore = jnp.zeros((ITERS, LANES), jnp.float32)
            aft = jnp.zeros((ITERS, LANES), jnp.float32)
            for q in range(min(per, n)):
                piece = recv_h[t // r + q]
                here = (lane >= q * r) & (lane < (q + 1) * r)
                fore = jnp.where(here, pltpu.roll(piece, (q * r - off) % LANES, 1), fore)
                aft = jnp.where(here, pltpu.roll(piece, (q * r - off - half) % LANES, 1), aft)
            at = pl.ds(top + t, LANES)
            hrow[pl.ds(0, ITERS), at] = -fore
            hrow[pl.ds(ITERS, ITERS), at] = -aft
    sub = lax.broadcasted_iota(jnp.int32, (SUB, 1), 0)
    negc[pl.ds(0, SUB), :] = jnp.where(sub >= ITERS, hrow[...], 0.0)
    for t in range(0, nw, LANES):
        at = pl.ds(t, LANES)
        ring = hrow[:, at]
        turned = ring
        for s in range(1, SUB):
            turned = jnp.where(phase == s, pltpu.roll(ring, s, 0), turned)
        hrow[:, at] = turned

    loads[7].wait()
    loads[8].wait()
    for k in order:
        copies(2, k, True).wait_recv()
        copies(3, k, True).wait_recv()

    def filled(r, value, at):
        ahead = sub + (r - SUB) - finish
        return jnp.where((ahead >= 0) & (ahead < ITERS), hrow[:, at], value)

    for r, top, src in ((rs, 0, recv_s), (ri, nx, recv_i)):
        per = LANES // r
        for t in range(0, n * r, LANES):
            at = pl.ds(top + t, LANES)
            for b in range(0, width, LANES):
                stack = [src[t // r + q, :, pl.ds(b, LANES)] for q in range(per)]
                turned = jnp.concatenate(stack, axis=0).T
                for i in range(0, LANES, SUB):
                    down = SUB + b + i
                    negc[pl.ds(down, SUB), at] = filled(down, -turned[i:i + SUB], at)
            negc[pl.ds(SUB + width, SUB), at] = filled(
                SUB + width, jnp.zeros((SUB, LANES), jnp.float32), at
            )

    for it in range(ITERS):
        last = it == ITERS - 1
        if it == 0:
            for r in range(0, rows, ROWS):
                at = pl.ds(r, ROWS)
                rhs[at, :] = negc[at, :].astype(jnp.bfloat16)
        else:
            for t in range(0, nw, TILE):
                to = pl.ds(t, TILE)
                w[:, to] = dot(g[...], ab[:, to])
                known = c if t < nx else negc
                for r in range(0, rows, ROWS):
                    at = pl.ds(r, ROWS)
                    rhs[at, to] = (known[at, to] + scaled(w[at, to])).astype(jnp.bfloat16)
        for t in range(0, nw, TILE):
            to = pl.ds(t, TILE)
            w[:, to] = dot(rhs[...], kt[:, to])
            for r in range(0, rows, ROWS):
                at = pl.ds(r, ROWS)
                wb[at, to] = w[at, to].astype(jnp.bfloat16)
        if last:
            primal = jnp.zeros((SUB, LANES), jnp.float32)
            dual = jnp.zeros((SUB, LANES), jnp.float32)
        for t in range(0, nx, TILE):
            to = pl.ds(t, TILE)
            pred[:, to] = dot(wb[...], abt[:, to])
            for r in range(0, rows, ROWS):
                at = pl.ds(r, ROWS)
                q = pred[at, to]
                link[pl.ds(SUB + r, ROWS), to] = q + v[at, to] if it else q
            for r in range(0, rows, ROWS):
                at = pl.ds(r, ROWS)
                x = w[at, to]
                own = x + y[at, to] if it else x
                znew = 0.5 * (own + link[pl.ds(SUB + r - 1, ROWS), to])
                zn[at, to] = znew
                if not last:
                    ynew = own - znew
                    y[at, to] = ynew
                    c[at, to] = negc[at, to] + scaled(znew - ynew)
                    if it == ITERS - 2:
                        z[at, to] = znew
            if not last:
                for r in range(0, rows, ROWS):
                    at = pl.ds(r, ROWS)
                    znext = zn[pl.ds(r + 1, ROWS), to]
                    vnew = link[pl.ds(SUB + r, ROWS), to] - znext
                    v[at, to] = vnew
                    g[at, to] = (znext - vnew).astype(jnp.bfloat16)
            else:
                for r in range(SUB, SUB + width, SUB):
                    at = pl.ds(r, SUB)
                    active = sub + (base + r - SUB) < period
                    znew = zn[at, to]
                    znext = zn[pl.ds(r + 1, SUB), to]
                    miss = (w[at, to] - znew) ** 2 + (pred[at, to] - znext) ** 2
                    change = znew - z[at, to]
                    miss = jnp.where(active, miss, 0.0)
                    change = jnp.where(active, change * change, 0.0)
                    for b in range(0, TILE, LANES):
                        primal = primal + miss[:, b:b + LANES]
                        dual = dual + change[:, b:b + LANES]

    part[pl.ds(0, 1), :] = jnp.sum(primal, axis=0, keepdims=True)
    part[pl.ds(1, 1), :] = RHO * RHO * jnp.sum(dual, axis=0, keepdims=True)
    recv_p[me] = part[...]
    for k in order:
        copies(0, k).start()

    for b in range(0, width, LANES):
        to = pl.ds(b, LANES)
        lane = lax.broadcasted_iota(jnp.int32, (1, LANES), 1)
        active = lane + (base + b) < period
        for t in range(0, nw, LANES):
            value = jnp.where(active, w[pl.ds(SUB + b, LANES), pl.ds(t, LANES)].T, 0.0)
            if t < nx:
                xo[pl.ds(t, LANES), to] = value
                zo[pl.ds(t, LANES), to] = jnp.where(
                    active, zn[pl.ds(SUB + b, LANES), pl.ds(t, LANES)].T, 0.0
                )
            else:
                uo[pl.ds(t - nx, LANES), to] = value
    outs = [
        pltpu.make_async_copy(xo, x_out, out_sem.at[0]),
        pltpu.make_async_copy(uo, u_out, out_sem.at[1]),
        pltpu.make_async_copy(zo, z_out, out_sem.at[2]),
    ]
    for copy in outs:
        copy.start()
    for k in order:
        copies(0, k, True).wait_recv()
    total = recv_p[0]
    for s in range(1, n):
        total = total + recv_p[s]
    top = jnp.sqrt(jnp.broadcast_to(jnp.sum(total[:1], keepdims=True), (SUB, LANES)))
    low = jnp.sqrt(jnp.broadcast_to(jnp.sum(total[1:], keepdims=True), (SUB, LANES)))
    norm_out[0] = jnp.max(top)
    norm_out[1] = jnp.max(low)
    for copy in outs:
        copy.wait()
    for kind in range(4):
        for k in order:
            copies(kind, k).wait_send()


def local(a, b, kkt, lin_state, lin_input, block_start, period):
    n = lax.axis_size("section")
    width = lin_state.shape[1] // n
    rows = width + 2 * SUB
    nx, nu = b.shape
    nw = nx + nu
    rs, ri = lin_state.shape[0], lin_input.shape[0]
    f32, bf16 = jnp.float32, jnp.bfloat16
    anyspec = pl.BlockSpec(memory_space=pl.ANY)
    smem = pl.BlockSpec(memory_space=pltpu.SMEM)
    vmem = pltpu.VMEM
    return pl.pallas_call(
        functools.partial(kernel, n, width),
        name="admm",
        out_shape=(
            jax.ShapeDtypeStruct((nx, width), f32),
            jax.ShapeDtypeStruct((nu, width), f32),
            jax.ShapeDtypeStruct((nx, width), f32),
            jax.ShapeDtypeStruct((2,), f32),
        ),
        in_specs=[anyspec] * 7,
        out_specs=(anyspec, anyspec, anyspec, smem),
        scratch_shapes=[
            vmem((nx, nw), bf16), vmem((nw, nx), bf16), vmem((nw, nw), bf16), vmem((nw, nw), bf16),
            vmem(lin_state.shape, f32), vmem(lin_input.shape, f32),
            vmem((n, rs, width), f32), vmem((n, ri, width), f32),
            vmem((LANES, CHUNK), f32),
            vmem((n, ITERS, LANES), f32), vmem((n, ITERS, LANES), f32), vmem((SUB, nw), f32),
            vmem((rows, nw), f32), vmem((rows, nw), bf16), vmem((rows, nw), f32),
            vmem((rows, nw), bf16), vmem((rows, nx), f32),
            vmem((rows + SUB, nx), f32), vmem((rows + SUB, nx), f32),
            vmem((rows, nx), f32), vmem((rows, nx), f32), vmem((rows, nx), f32), vmem((rows, nx), f32),
            vmem((rows, nx), bf16),
            vmem((nx, width), f32), vmem((nu, width), f32), vmem((nx, width), f32),
            vmem((2, LANES), f32), vmem((n, 2, LANES), f32),
            pltpu.SMEM((1,), jnp.int32), pltpu.SMEM((1,), jnp.int32),
            pltpu.SemaphoreType.DMA((9,)),
            pltpu.SemaphoreType.DMA((4, n)), pltpu.SemaphoreType.DMA((4, n)),
            pltpu.SemaphoreType.DMA((3,)),
        ],
        compiler_params=pltpu.CompilerParams(
            collective_id=0, has_side_effects=True, vmem_limit_bytes=62000000
        ),
    )(a, b, kkt, lin_state, lin_input, block_start, period)


def solution(mesh):
    return jax.shard_map(
        local,
        mesh=mesh,
        in_specs=(
            P("plant", None),
            P("plant", None),
            P("plant", None),
            P(("plant", "section"), None),
            P(("plant", "section"), None),
            P("plant"),
            P("plant"),
        ),
        out_specs=(P("plant", "section"), P("plant", "section"), P("plant", "section"), P("plant")),
        check_vma=False,
    )
```

```python
import functools

import jax
import jax.numpy as jnp
from jax import lax
from jax.experimental import pallas as pl
from jax.experimental.pallas import tpu as pltpu
from jax.sharding import PartitionSpec as P

ITERS = 4
RHO = 1.0
LANES = 128
SUB = 8
CHUNK = 512
TILE = 256
ROWS = 16
NT = (((1,), (1,)), ((), ()))


def dot(a, b):
    return jnp.dot(a, b, preferred_element_type=jnp.float32)


def scaled(value):
    return value if RHO == 1.0 else RHO * value


def partner(me, k, n, sign):
    if n & (n - 1):
        return lax.rem(me + sign * k + n, n)
    other = me
    for bit in range(n.bit_length()):
        if (k >> bit) & 1:
            other = other + (1 - 2 * ((me // (1 << bit)) % 2)) * (1 << bit)
    return other


def kernel(
    n, width,
    a_hbm, b_hbm, k_hbm, cs_hbm, ci_hbm, start_ref, period_ref,
    xo, uo, zo, norm_out,
    ab, abt, kkt, kt, cs, ci, recv_s, recv_i, cpad, hsend, recv_h, hrow,
    negc, rhs, w, wb, pred, link, zn, y, v, c, z, g, part, recv_p,
    load_sem, send_sem, recv_sem,
):
    me = lax.axis_index("section")
    nx = a_hbm.shape[0]
    nu = b_hbm.shape[1]
    nw = nx + nu
    rs, ri = cs.shape[0], ci.shape[0]
    rows = width + 2 * SUB
    half = LANES // 2

    def cols(i):
        return pl.ds(pl.multiple_of(i * width, LANES), width)

    loads = [
        pltpu.make_async_copy(cs_hbm, cs, load_sem.at[0]),
        pltpu.make_async_copy(ci_hbm, ci, load_sem.at[1]),
        pltpu.make_async_copy(a_hbm, ab.at[:, pl.ds(0, nx)], load_sem.at[2]),
        pltpu.make_async_copy(b_hbm, ab.at[:, pl.ds(nx, nu)], load_sem.at[3]),
        pltpu.make_async_copy(k_hbm, kkt, load_sem.at[4]),
        pltpu.make_async_copy(cs_hbm.at[:, cols(me)], recv_s.at[me], load_sem.at[5]),
        pltpu.make_async_copy(ci_hbm.at[:, cols(me)], recv_i.at[me], load_sem.at[6]),
    ]
    barrier = pltpu.get_barrier_semaphore()
    for k in range(1, n):
        pl.semaphore_signal(barrier, inc=1, device_id={"section": partner(me, k, n, 1)})
    for copy in loads:
        copy.start()

    def copies(kind, k, incoming=False):
        to = partner(me, k, n, 1)
        if kind == 0:
            src, dst = part, recv_p
        elif kind == 1:
            src, dst = hsend.at[to], recv_h
        elif kind == 2:
            src, dst = cs.at[:, cols(to)], recv_s
        else:
            src, dst = ci.at[:, cols(to)], recv_i
        slot = partner(me, k, n, -1) if incoming else me
        return pltpu.make_async_remote_copy(
            src_ref=src, dst_ref=dst.at[slot], send_sem=send_sem.at[kind, k],
            recv_sem=recv_sem.at[kind, slot], device_id={"section": to},
        )

    order = list(range(n // 2, n)) + list(range(n // 2 - 1, 0, -1))

    for copy in loads[:2]:
        copy.wait()
    start = start_ref[0]
    period = period_ref[0]

    row = lax.broadcasted_iota(jnp.int32, (n * SUB, 1), 0)
    late = row >= n * ITERS
    row = jnp.where(late, row - n * ITERS, row)
    block = row // ITERS - start
    block = jnp.where(block < 0, block + n, block)
    base = block * width
    item = row % ITERS
    ahead = base + jnp.minimum(period - base, width) + item
    ahead = jnp.where(ahead >= period, ahead - period, ahead)
    behind = base + item - ITERS
    behind = jnp.where(behind < 0, behind + period, behind)
    place = jnp.where(late, behind, ahead) + start * width
    place = jnp.where(place >= n * width, place - n * width, place)

    cpad[...] = jnp.zeros_like(cpad)

    def pick(j, total):
        at = pl.ds(pl.multiple_of(j * CHUNK, CHUNK), CHUNK)
        cpad[pl.ds(0, rs), :] = cs[:, at]
        cpad[pl.ds(rs, ri), :] = ci[:, at]
        column = lax.broadcasted_iota(jnp.int32, (n * SUB, CHUNK), 1) + j * CHUNK
        onehot = jnp.where(column == place, 1.0, 0.0).astype(jnp.bfloat16)
        rest = cpad[...]
        for _ in range(3):
            piece = rest.astype(jnp.bfloat16)
            rest = rest - piece.astype(jnp.float32)
            total = total + lax.dot_general(onehot, piece, NT, preferred_element_type=jnp.float32)
        return total

    picked = lax.fori_loop(
        0, cs.shape[1] // CHUNK, pick, jnp.zeros((n * SUB, LANES), jnp.float32)
    )
    packed = picked[:n * ITERS] + pltpu.roll(picked[n * ITERS:], half, 1)
    hsend[...] = packed.reshape(n, ITERS, LANES)
    recv_h[me] = hsend[me]

    pl.semaphore_wait(barrier, n - 1)
    for k in order:
        copies(1, k).start()
    for k in order:
        copies(2, k).start()
        copies(3, k).start()

    for copy in loads[2:5]:
        copy.wait()
    abt[...] = ab[...].T
    kt[...] = kkt[...].T
    link[pl.ds(0, SUB), :] = jnp.zeros((SUB, nx), jnp.float32)
    zn[pl.ds(rows, SUB), :] = jnp.zeros((SUB, nx), jnp.float32)

    mine = me - start
    mine = jnp.where(mine < 0, mine + n, mine)
    base = mine * width
    finish = jnp.minimum(period - base, width)

    for k in order:
        copies(1, k, True).wait_recv()

    lane = lax.broadcasted_iota(jnp.int32, (ITERS, LANES), 1)
    phase = (finish + 2 * width) % SUB
    for r, top in ((rs, 0), (ri, nx)):
        off = 0 if top == 0 else rs
        per = LANES // r
        for t in range(0, n * r, LANES):
            fore = jnp.zeros((ITERS, LANES), jnp.float32)
            aft = jnp.zeros((ITERS, LANES), jnp.float32)
            for q in range(min(per, n)):
                piece = recv_h[t // r + q]
                here = (lane >= q * r) & (lane < (q + 1) * r)
                fore = jnp.where(here, pltpu.roll(piece, (q * r - off) % LANES, 1), fore)
                aft = jnp.where(here, pltpu.roll(piece, (q * r - off - half) % LANES, 1), aft)
            at = pl.ds(top + t, LANES)
            hrow[pl.ds(0, ITERS), at] = -fore
            hrow[pl.ds(ITERS, ITERS), at] = -aft
    sub = lax.broadcasted_iota(jnp.int32, (SUB, 1), 0)
    negc[pl.ds(0, SUB), :] = jnp.where(sub >= ITERS, hrow[...], 0.0)
    for t in range(0, nw, LANES):
        at = pl.ds(t, LANES)
        ring = hrow[:, at]
        turned = ring
        for s in range(1, SUB):
            turned = jnp.where(phase == s, pltpu.roll(ring, s, 0), turned)
        hrow[:, at] = turned

    loads[5].wait()
    loads[6].wait()
    for k in order:
        copies(2, k, True).wait_recv()
        copies(3, k, True).wait_recv()

    def filled(r, value, at):
        ahead = sub + (r - SUB) - finish
        return jnp.where((ahead >= 0) & (ahead < ITERS), hrow[:, at], value)

    for r, top, src in ((rs, 0, recv_s), (ri, nx, recv_i)):
        per = LANES // r
        for t in range(0, n * r, LANES):
            at = pl.ds(top + t, LANES)
            for b in range(0, width, LANES):
                stack = [src[t // r + q, :, pl.ds(b, LANES)] for q in range(per)]
                turned = jnp.concatenate(stack, axis=0).T
                for i in range(0, LANES, SUB):
                    down = SUB + b + i
                    negc[pl.ds(down, SUB), at] = filled(down, -turned[i:i + SUB], at)
            negc[pl.ds(SUB + width, SUB), at] = filled(
                SUB + width, jnp.zeros((SUB, LANES), jnp.float32), at
            )

    for it in range(ITERS):
        last = it == ITERS - 1
        if it == 0:
            for r in range(0, rows, ROWS):
                at = pl.ds(r, ROWS)
                rhs[at, :] = negc[at, :].astype(jnp.bfloat16)
        else:
            for t in range(0, nw, TILE):
                to = pl.ds(t, TILE)
                w[:, to] = dot(g[...], ab[:, to])
                known = c if t < nx else negc
                for r in range(0, rows, ROWS):
                    at = pl.ds(r, ROWS)
                    rhs[at, to] = (known[at, to] + scaled(w[at, to])).astype(jnp.bfloat16)
        for t in range(0, nw, TILE):
            to = pl.ds(t, TILE)
            w[:, to] = dot(rhs[...], kt[:, to])
            for r in range(0, rows, ROWS):
                at = pl.ds(r, ROWS)
                wb[at, to] = w[at, to].astype(jnp.bfloat16)
        if last:
            primal = jnp.zeros((SUB, LANES), jnp.float32)
            dual = jnp.zeros((SUB, LANES), jnp.float32)
        for t in range(0, nx, TILE):
            to = pl.ds(t, TILE)
            pred[:, to] = dot(wb[...], abt[:, to])
            for r in range(0, rows, ROWS):
                at = pl.ds(r, ROWS)
                q = pred[at, to]
                link[pl.ds(SUB + r, ROWS), to] = q + v[at, to] if it else q
            for r in range(0, rows, ROWS):
                at = pl.ds(r, ROWS)
                x = w[at, to]
                own = x + y[at, to] if it else x
                znew = 0.5 * (own + link[pl.ds(SUB + r - 1, ROWS), to])
                zn[at, to] = znew
                if not last:
                    ynew = own - znew
                    y[at, to] = ynew
                    c[at, to] = negc[at, to] + scaled(znew - ynew)
                    if it == ITERS - 2:
                        z[at, to] = znew
            if not last:
                for r in range(0, rows, ROWS):
                    at = pl.ds(r, ROWS)
                    znext = zn[pl.ds(r + 1, ROWS), to]
                    vnew = link[pl.ds(SUB + r, ROWS), to] - znext
                    v[at, to] = vnew
                    g[at, to] = (znext - vnew).astype(jnp.bfloat16)
            else:
                for r in range(SUB, SUB + width, SUB):
                    at = pl.ds(r, SUB)
                    active = sub + (base + r - SUB) < period
                    znew = zn[at, to]
                    znext = zn[pl.ds(r + 1, SUB), to]
                    miss = (w[at, to] - znew) ** 2 + (pred[at, to] - znext) ** 2
                    change = znew - z[at, to]
                    miss = jnp.where(active, miss, 0.0)
                    change = jnp.where(active, change * change, 0.0)
                    for b in range(0, TILE, LANES):
                        primal = primal + miss[:, b:b + LANES]
                        dual = dual + change[:, b:b + LANES]

    part[pl.ds(0, 1), :] = jnp.sum(primal, axis=0, keepdims=True)
    part[pl.ds(1, 1), :] = RHO * RHO * jnp.sum(dual, axis=0, keepdims=True)
    recv_p[me] = part[...]
    for k in order:
        copies(0, k).start()

    for b in range(0, width, LANES):
        to = pl.ds(b, LANES)
        lane = lax.broadcasted_iota(jnp.int32, (1, LANES), 1)
        active = lane + (base + b) < period
        for t in range(0, nw, LANES):
            value = jnp.where(active, w[pl.ds(SUB + b, LANES), pl.ds(t, LANES)].T, 0.0)
            if t < nx:
                xo[pl.ds(t, LANES), to] = value
                zo[pl.ds(t, LANES), to] = jnp.where(
                    active, zn[pl.ds(SUB + b, LANES), pl.ds(t, LANES)].T, 0.0
                )
            else:
                uo[pl.ds(t - nx, LANES), to] = value
    for k in order:
        copies(0, k, True).wait_recv()
    total = recv_p[0]
    for s in range(1, n):
        total = total + recv_p[s]
    top = jnp.sqrt(jnp.broadcast_to(jnp.sum(total[:1], keepdims=True), (SUB, LANES)))
    low = jnp.sqrt(jnp.broadcast_to(jnp.sum(total[1:], keepdims=True), (SUB, LANES)))
    norm_out[0] = jnp.max(top)
    norm_out[1] = jnp.max(low)
    for kind in range(4):
        for k in order:
            copies(kind, k).wait_send()


def store(*refs):
    sem = refs[-1]
    half = (len(refs) - 1) // 2
    moves = [
        pltpu.make_async_copy(refs[i], refs[half + i], sem.at[i]) for i in range(half)
    ]
    for move in moves:
        move.start()
    for move in moves:
        move.wait()


def local(a, b, kkt, lin_state, lin_input, block_start, period):
    n = lax.axis_size("section")
    width = lin_state.shape[1] // n
    rows = width + 2 * SUB
    nx, nu = b.shape
    nw = nx + nu
    rs, ri = lin_state.shape[0], lin_input.shape[0]
    f32, bf16 = jnp.float32, jnp.bfloat16
    anyspec = pl.BlockSpec(memory_space=pl.ANY)
    smem = pl.BlockSpec(memory_space=pltpu.SMEM)
    vspec = pl.BlockSpec(memory_space=pltpu.VMEM)
    hbm = pl.BlockSpec(memory_space=pltpu.HBM)
    vmem = pltpu.VMEM
    inputs = [
        pltpu.with_memory_space_constraint(value, pltpu.HBM)
        for value in (a, b, kkt, lin_state, lin_input)
    ]
    results = pl.pallas_call(
        functools.partial(kernel, n, width),
        name="admm",
        out_shape=(
            jax.ShapeDtypeStruct((nx, width), f32),
            jax.ShapeDtypeStruct((nu, width), f32),
            jax.ShapeDtypeStruct((nx, width), f32),
            jax.ShapeDtypeStruct((2,), f32),
        ),
        in_specs=[hbm] * 5 + [smem] * 2,
        out_specs=(vspec, vspec, vspec, smem),
        scratch_shapes=[
            vmem((nx, nw), bf16), vmem((nw, nx), bf16), vmem((nw, nw), bf16), vmem((nw, nw), bf16),
            vmem(lin_state.shape, f32), vmem(lin_input.shape, f32),
            vmem((n, rs, width), f32), vmem((n, ri, width), f32),
            vmem((LANES, CHUNK), f32),
            vmem((n, ITERS, LANES), f32), vmem((n, ITERS, LANES), f32), vmem((SUB, nw), f32),
            vmem((rows, nw), f32), vmem((rows, nw), bf16), vmem((rows, nw), f32),
            vmem((rows, nw), bf16), vmem((rows, nx), f32),
            vmem((rows + SUB, nx), f32), vmem((rows + SUB, nx), f32),
            vmem((rows, nx), f32), vmem((rows, nx), f32), vmem((rows, nx), f32), vmem((rows, nx), f32),
            vmem((rows, nx), bf16),
            vmem((2, LANES), f32), vmem((n, 2, LANES), f32),
            pltpu.SemaphoreType.DMA((7,)),
            pltpu.SemaphoreType.DMA((4, n)), pltpu.SemaphoreType.DMA((4, n)),
        ],
        compiler_params=pltpu.CompilerParams(
            collective_id=0, has_side_effects=True, vmem_limit_bytes=24000000
        ),
    )(*inputs, block_start, period)
    return pl.pallas_call(
        store,
        name="store",
        out_shape=tuple(jax.ShapeDtypeStruct(r.shape, r.dtype) for r in results),
        in_specs=[anyspec] * 4,
        out_specs=(anyspec,) * 4,
        scratch_shapes=[pltpu.SemaphoreType.DMA((4,))],
        compiler_params=pltpu.CompilerParams(vmem_limit_bytes=4000000),
    )(*results)


def solution(mesh):
    return jax.shard_map(
        local,
        mesh=mesh,
        in_specs=(
            P("plant", None),
            P("plant", None),
            P("plant", None),
            P(("plant", "section"), None),
            P(("plant", "section"), None),
            P("plant"),
            P("plant"),
        ),
        out_specs=(P("plant", "section"), P("plant", "section"), P("plant", "section"), P("plant")),
        check_vma=False,
    )
```

```python
import functools

import jax
import jax.numpy as jnp
from jax import lax
from jax.experimental import pallas as pl
from jax.experimental.pallas import tpu as pltpu
from jax.sharding import PartitionSpec as P

ITERS = 4
RHO = 1.0
LANES = 128
SUB = 8
CHUNK = 512
TILE = 256
ROWS = 16
NT = (((1,), (1,)), ((), ()))


def dot(a, b):
    return jnp.dot(a, b, preferred_element_type=jnp.float32)


def scaled(value):
    return value if RHO == 1.0 else RHO * value


def partner(me, k, n, sign):
    if n & (n - 1):
        return lax.rem(me + sign * k + n, n)
    other = me
    for bit in range(n.bit_length()):
        if (k >> bit) & 1:
            other = other + (1 - 2 * ((me // (1 << bit)) % 2)) * (1 << bit)
    return other


def kernel(
    n, width,
    a_hbm, b_hbm, k_hbm, cs_hbm, ci_hbm, start_ref, period_ref,
    xo, uo, zo, total_out,
    ab, abt, kkt, kt, cs, ci, recv_s, recv_i, cpad, hsend, recv_h, hrow,
    negc, rhs, w, wb, pred, link, zn, y, v, c, z, g, part, recv_p,
    load_sem, send_sem, recv_sem,
):
    me = lax.axis_index("section")
    nx = a_hbm.shape[0]
    nu = b_hbm.shape[1]
    nw = nx + nu
    rs, ri = cs.shape[0], ci.shape[0]
    rows = width + 2 * SUB
    half = LANES // 2

    def cols(i):
        return pl.ds(pl.multiple_of(i * width, LANES), width)

    loads = [
        pltpu.make_async_copy(cs_hbm, cs, load_sem.at[0]),
        pltpu.make_async_copy(ci_hbm, ci, load_sem.at[1]),
        pltpu.make_async_copy(a_hbm, ab.at[:, pl.ds(0, nx)], load_sem.at[2]),
        pltpu.make_async_copy(b_hbm, ab.at[:, pl.ds(nx, nu)], load_sem.at[3]),
        pltpu.make_async_copy(k_hbm, kkt, load_sem.at[4]),
        pltpu.make_async_copy(cs_hbm.at[:, cols(me)], recv_s.at[me], load_sem.at[5]),
        pltpu.make_async_copy(ci_hbm.at[:, cols(me)], recv_i.at[me], load_sem.at[6]),
    ]
    barrier = pltpu.get_barrier_semaphore()
    for k in range(1, n):
        pl.semaphore_signal(barrier, inc=1, device_id={"section": partner(me, k, n, 1)})
    for copy in loads:
        copy.start()

    def copies(kind, k, incoming=False):
        to = partner(me, k, n, 1)
        if kind == 0:
            src, dst = part, recv_p
        elif kind == 1:
            src, dst = hsend.at[to], recv_h
        elif kind == 2:
            src, dst = cs.at[:, cols(to)], recv_s
        else:
            src, dst = ci.at[:, cols(to)], recv_i
        slot = partner(me, k, n, -1) if incoming else me
        return pltpu.make_async_remote_copy(
            src_ref=src, dst_ref=dst.at[slot], send_sem=send_sem.at[kind, k],
            recv_sem=recv_sem.at[kind, slot], device_id={"section": to},
        )

    order = list(range(n // 2, n)) + list(range(n // 2 - 1, 0, -1))

    for copy in loads[:2]:
        copy.wait()
    start = start_ref[0]
    period = period_ref[0]

    row = lax.broadcasted_iota(jnp.int32, (n * SUB, 1), 0)
    late = row >= n * ITERS
    row = jnp.where(late, row - n * ITERS, row)
    block = row // ITERS - start
    block = jnp.where(block < 0, block + n, block)
    base = block * width
    item = row % ITERS
    ahead = base + jnp.minimum(period - base, width) + item
    ahead = jnp.where(ahead >= period, ahead - period, ahead)
    behind = base + item - ITERS
    behind = jnp.where(behind < 0, behind + period, behind)
    place = jnp.where(late, behind, ahead) + start * width
    place = jnp.where(place >= n * width, place - n * width, place)

    cpad[...] = jnp.zeros_like(cpad)

    def pick(j, total):
        at = pl.ds(pl.multiple_of(j * CHUNK, CHUNK), CHUNK)
        cpad[pl.ds(0, rs), :] = cs[:, at]
        cpad[pl.ds(rs, ri), :] = ci[:, at]
        column = lax.broadcasted_iota(jnp.int32, (n * SUB, CHUNK), 1) + j * CHUNK
        onehot = jnp.where(column == place, 1.0, 0.0).astype(jnp.bfloat16)
        rest = cpad[...]
        for _ in range(3):
            piece = rest.astype(jnp.bfloat16)
            rest = rest - piece.astype(jnp.float32)
            total = total + lax.dot_general(onehot, piece, NT, preferred_element_type=jnp.float32)
        return total

    picked = lax.fori_loop(
        0, cs.shape[1] // CHUNK, pick, jnp.zeros((n * SUB, LANES), jnp.float32)
    )
    packed = picked[:n * ITERS] + pltpu.roll(picked[n * ITERS:], half, 1)
    hsend[...] = packed.reshape(n, ITERS, LANES)
    recv_h[me] = hsend[me]

    pl.semaphore_wait(barrier, n - 1)
    for k in order:
        copies(1, k).start()
    for k in order:
        copies(2, k).start()
        copies(3, k).start()

    for copy in loads[2:5]:
        copy.wait()
    abt[...] = ab[...].T
    kt[...] = kkt[...].T
    link[pl.ds(0, SUB), :] = jnp.zeros((SUB, nx), jnp.float32)
    zn[pl.ds(rows, SUB), :] = jnp.zeros((SUB, nx), jnp.float32)

    mine = me - start
    mine = jnp.where(mine < 0, mine + n, mine)
    base = mine * width
    finish = jnp.minimum(period - base, width)

    for k in order:
        copies(1, k, True).wait_recv()

    lane = lax.broadcasted_iota(jnp.int32, (ITERS, LANES), 1)
    phase = (finish + 2 * width) % SUB
    for r, top in ((rs, 0), (ri, nx)):
        off = 0 if top == 0 else rs
        per = LANES // r
        for t in range(0, n * r, LANES):
            fore = jnp.zeros((ITERS, LANES), jnp.float32)
            aft = jnp.zeros((ITERS, LANES), jnp.float32)
            for q in range(min(per, n)):
                piece = recv_h[t // r + q]
                here = (lane >= q * r) & (lane < (q + 1) * r)
                fore = jnp.where(here, pltpu.roll(piece, (q * r - off) % LANES, 1), fore)
                aft = jnp.where(here, pltpu.roll(piece, (q * r - off - half) % LANES, 1), aft)
            at = pl.ds(top + t, LANES)
            hrow[pl.ds(0, ITERS), at] = -fore
            hrow[pl.ds(ITERS, ITERS), at] = -aft
    sub = lax.broadcasted_iota(jnp.int32, (SUB, 1), 0)
    negc[pl.ds(0, SUB), :] = jnp.where(sub >= ITERS, hrow[...], 0.0)
    for t in range(0, nw, LANES):
        at = pl.ds(t, LANES)
        ring = hrow[:, at]
        turned = ring
        for s in range(1, SUB):
            turned = jnp.where(phase == s, pltpu.roll(ring, s, 0), turned)
        hrow[:, at] = turned

    loads[5].wait()
    loads[6].wait()
    for k in order:
        copies(2, k, True).wait_recv()
        copies(3, k, True).wait_recv()

    def filled(r, value, at):
        ahead = sub + (r - SUB) - finish
        return jnp.where((ahead >= 0) & (ahead < ITERS), hrow[:, at], value)

    for r, top, src in ((rs, 0, recv_s), (ri, nx, recv_i)):
        per = LANES // r
        for t in range(0, n * r, LANES):
            at = pl.ds(top + t, LANES)
            for b in range(0, width, LANES):
                stack = [src[t // r + q, :, pl.ds(b, LANES)] for q in range(per)]
                turned = jnp.concatenate(stack, axis=0).T
                for i in range(0, LANES, SUB):
                    down = SUB + b + i
                    negc[pl.ds(down, SUB), at] = filled(down, -turned[i:i + SUB], at)
            negc[pl.ds(SUB + width, SUB), at] = filled(
                SUB + width, jnp.zeros((SUB, LANES), jnp.float32), at
            )

    for it in range(ITERS):
        last = it == ITERS - 1
        if it == 0:
            for r in range(0, rows, ROWS):
                at = pl.ds(r, ROWS)
                rhs[at, :] = negc[at, :].astype(jnp.bfloat16)
        else:
            for t in range(0, nw, TILE):
                to = pl.ds(t, TILE)
                w[:, to] = dot(g[...], ab[:, to])
                known = c if t < nx else negc
                for r in range(0, rows, ROWS):
                    at = pl.ds(r, ROWS)
                    rhs[at, to] = (known[at, to] + scaled(w[at, to])).astype(jnp.bfloat16)
        for t in range(0, nw, TILE):
            to = pl.ds(t, TILE)
            w[:, to] = dot(rhs[...], kt[:, to])
            for r in range(0, rows, ROWS):
                at = pl.ds(r, ROWS)
                wb[at, to] = w[at, to].astype(jnp.bfloat16)
        if last:
            primal = jnp.zeros((SUB, LANES), jnp.float32)
            dual = jnp.zeros((SUB, LANES), jnp.float32)
        for t in range(0, nx, TILE):
            to = pl.ds(t, TILE)
            pred[:, to] = dot(wb[...], abt[:, to])
            for r in range(0, rows, ROWS):
                at = pl.ds(r, ROWS)
                q = pred[at, to]
                link[pl.ds(SUB + r, ROWS), to] = q + v[at, to] if it else q
            for r in range(0, rows, ROWS):
                at = pl.ds(r, ROWS)
                x = w[at, to]
                own = x + y[at, to] if it else x
                znew = 0.5 * (own + link[pl.ds(SUB + r - 1, ROWS), to])
                zn[at, to] = znew
                if not last:
                    ynew = own - znew
                    y[at, to] = ynew
                    c[at, to] = negc[at, to] + scaled(znew - ynew)
                    if it == ITERS - 2:
                        z[at, to] = znew
            if not last:
                for r in range(0, rows, ROWS):
                    at = pl.ds(r, ROWS)
                    znext = zn[pl.ds(r + 1, ROWS), to]
                    vnew = link[pl.ds(SUB + r, ROWS), to] - znext
                    v[at, to] = vnew
                    g[at, to] = (znext - vnew).astype(jnp.bfloat16)
            else:
                for r in range(SUB, SUB + width, SUB):
                    at = pl.ds(r, SUB)
                    active = sub + (base + r - SUB) < period
                    znew = zn[at, to]
                    znext = zn[pl.ds(r + 1, SUB), to]
                    miss = (w[at, to] - znew) ** 2 + (pred[at, to] - znext) ** 2
                    change = znew - z[at, to]
                    miss = jnp.where(active, miss, 0.0)
                    change = jnp.where(active, change * change, 0.0)
                    for b in range(0, TILE, LANES):
                        primal = primal + miss[:, b:b + LANES]
                        dual = dual + change[:, b:b + LANES]

    part[pl.ds(0, 1), :] = jnp.sum(primal, axis=0, keepdims=True)
    part[pl.ds(1, 1), :] = RHO * RHO * jnp.sum(dual, axis=0, keepdims=True)
    recv_p[me] = part[...]
    for k in order:
        copies(0, k).start()

    for b in range(0, width, LANES):
        to = pl.ds(b, LANES)
        lane = lax.broadcasted_iota(jnp.int32, (1, LANES), 1)
        active = lane + (base + b) < period
        for t in range(0, nw, LANES):
            value = jnp.where(active, w[pl.ds(SUB + b, LANES), pl.ds(t, LANES)].T, 0.0)
            if t < nx:
                xo[pl.ds(t, LANES), to] = value
                zo[pl.ds(t, LANES), to] = jnp.where(
                    active, zn[pl.ds(SUB + b, LANES), pl.ds(t, LANES)].T, 0.0
                )
            else:
                uo[pl.ds(t - nx, LANES), to] = value
    for k in order:
        copies(0, k, True).wait_recv()
    total = recv_p[0]
    for s in range(1, n):
        total = total + recv_p[s]
    total_out[...] = total
    for kind in range(4):
        for k in order:
            copies(kind, k).wait_send()


def store(x, u, z, total, x_out, u_out, z_out, norm_out, norm, sem):
    moves = [
        pltpu.make_async_copy(src, dst, sem.at[i])
        for i, (src, dst) in enumerate(((x, x_out), (u, u_out), (z, z_out)))
    ]
    for move in moves:
        move.start()
    both = jnp.sum(total[...], axis=1, keepdims=True)
    both = jnp.sqrt(jnp.broadcast_to(both, (2, LANES)))
    norm[0] = jnp.max(both[:1])
    norm[1] = jnp.max(both[1:])
    last = pltpu.make_async_copy(norm, norm_out, sem.at[3])
    last.start()
    for move in moves:
        move.wait()
    last.wait()


def local(a, b, kkt, lin_state, lin_input, block_start, period):
    n = lax.axis_size("section")
    width = lin_state.shape[1] // n
    rows = width + 2 * SUB
    nx, nu = b.shape
    nw = nx + nu
    rs, ri = lin_state.shape[0], lin_input.shape[0]
    f32, bf16 = jnp.float32, jnp.bfloat16
    anyspec = pl.BlockSpec(memory_space=pl.ANY)
    smem = pl.BlockSpec(memory_space=pltpu.SMEM)
    vspec = pl.BlockSpec(memory_space=pltpu.VMEM)
    hbm = pl.BlockSpec(memory_space=pltpu.HBM)
    vmem = pltpu.VMEM
    inputs = [
        pltpu.with_memory_space_constraint(value, pltpu.HBM)
        for value in (a, b, kkt, lin_state, lin_input)
    ]
    results = pl.pallas_call(
        functools.partial(kernel, n, width),
        name="admm",
        out_shape=(
            jax.ShapeDtypeStruct((nx, width), f32),
            jax.ShapeDtypeStruct((nu, width), f32),
            jax.ShapeDtypeStruct((nx, width), f32),
            jax.ShapeDtypeStruct((2, LANES), f32),
        ),
        in_specs=[hbm] * 5 + [smem] * 2,
        out_specs=(vspec,) * 4,
        scratch_shapes=[
            vmem((nx, nw), bf16), vmem((nw, nx), bf16), vmem((nw, nw), bf16), vmem((nw, nw), bf16),
            vmem(lin_state.shape, f32), vmem(lin_input.shape, f32),
            vmem((n, rs, width), f32), vmem((n, ri, width), f32),
            vmem((LANES, CHUNK), f32),
            vmem((n, ITERS, LANES), f32), vmem((n, ITERS, LANES), f32), vmem((SUB, nw), f32),
            vmem((rows, nw), f32), vmem((rows, nw), bf16), vmem((rows, nw), f32),
            vmem((rows, nw), bf16), vmem((rows, nx), f32),
            vmem((rows + SUB, nx), f32), vmem((rows + SUB, nx), f32),
            vmem((rows, nx), f32), vmem((rows, nx), f32), vmem((rows, nx), f32), vmem((rows, nx), f32),
            vmem((rows, nx), bf16),
            vmem((2, LANES), f32), vmem((n, 2, LANES), f32),
            pltpu.SemaphoreType.DMA((7,)),
            pltpu.SemaphoreType.DMA((4, n)), pltpu.SemaphoreType.DMA((4, n)),
        ],
        compiler_params=pltpu.CompilerParams(
            collective_id=0, has_side_effects=True, vmem_limit_bytes=24000000
        ),
    )(*inputs, block_start, period)
    return pl.pallas_call(
        store,
        name="store",
        out_shape=tuple(jax.ShapeDtypeStruct(r.shape, f32) for r in results[:3])
        + (jax.ShapeDtypeStruct((2,), f32),),
        in_specs=[anyspec] * 3 + [vspec],
        out_specs=(anyspec,) * 4,
        scratch_shapes=[pltpu.SMEM((2,), f32), pltpu.SemaphoreType.DMA((4,))],
        compiler_params=pltpu.CompilerParams(vmem_limit_bytes=4000000),
    )(*results)


def solution(mesh):
    return jax.shard_map(
        local,
        mesh=mesh,
        in_specs=(
            P("plant", None),
            P("plant", None),
            P("plant", None),
            P(("plant", "section"), None),
            P(("plant", "section"), None),
            P("plant"),
            P("plant"),
        ),
        out_specs=(P("plant", "section"), P("plant", "section"), P("plant", "section"), P("plant")),
        check_vma=False,
    )
```

```python
import functools

import jax
import jax.numpy as jnp
from jax import lax
from jax.experimental import pallas as pl
from jax.experimental.pallas import tpu as pltpu
from jax.sharding import PartitionSpec as P

ITERS = 4
RHO = 1.0
LANES = 128
SUB = 8
CHUNK = 512
TILE = 256
ROWS = 16
NT = (((1,), (1,)), ((), ()))


def dot(a, b):
    return jnp.dot(a, b, preferred_element_type=jnp.float32)


def scaled(value):
    return value if RHO == 1.0 else RHO * value


def partner(me, k, n, sign):
    if n & (n - 1):
        return lax.rem(me + sign * k + n, n)
    other = me
    for bit in range(n.bit_length()):
        if (k >> bit) & 1:
            other = other + (1 - 2 * ((me // (1 << bit)) % 2)) * (1 << bit)
    return other


def kernel(
    n, width,
    a_hbm, b_hbm, k_hbm, cs_hbm, ci_hbm, start_ref, period_ref,
    xo, uo, zo, total_out,
    ab, abt, kkt, kt, cs, ci, recv_s, recv_i, cpad, hsend, recv_h, hrow,
    negc, rhs, w, wb, pred, link, zn, y, v, c, z, g, part, recv_p,
    load_sem, send_sem, recv_sem,
):
    me = lax.axis_index("section")
    nx = a_hbm.shape[0]
    nu = b_hbm.shape[1]
    nw = nx + nu
    rs, ri = cs.shape[0], ci.shape[0]
    rows = width + 2 * SUB
    half = LANES // 2

    def cols(i):
        return pl.ds(pl.multiple_of(i * width, LANES), width)

    loads = [
        pltpu.make_async_copy(cs_hbm, cs, load_sem.at[0]),
        pltpu.make_async_copy(ci_hbm, ci, load_sem.at[1]),
        pltpu.make_async_copy(a_hbm, ab.at[:, pl.ds(0, nx)], load_sem.at[2]),
        pltpu.make_async_copy(b_hbm, ab.at[:, pl.ds(nx, nu)], load_sem.at[3]),
        pltpu.make_async_copy(k_hbm, kkt, load_sem.at[4]),
        pltpu.make_async_copy(cs_hbm.at[:, cols(me)], recv_s.at[me], load_sem.at[5]),
        pltpu.make_async_copy(ci_hbm.at[:, cols(me)], recv_i.at[me], load_sem.at[6]),
    ]
    barrier = pltpu.get_barrier_semaphore()
    for k in range(1, n):
        pl.semaphore_signal(barrier, inc=1, device_id={"section": partner(me, k, n, 1)})
    for copy in loads:
        copy.start()

    def copies(kind, k, incoming=False):
        to = partner(me, k, n, 1)
        if kind == 0:
            src, dst = part, recv_p
        elif kind == 1:
            src, dst = hsend.at[to], recv_h
        elif kind == 2:
            src, dst = cs.at[:, cols(to)], recv_s
        else:
            src, dst = ci.at[:, cols(to)], recv_i
        slot = partner(me, k, n, -1) if incoming else me
        return pltpu.make_async_remote_copy(
            src_ref=src, dst_ref=dst.at[slot], send_sem=send_sem.at[kind, k],
            recv_sem=recv_sem.at[kind, slot], device_id={"section": to},
        )

    order = list(range(n // 2, n)) + list(range(n // 2 - 1, 0, -1))

    for copy in loads[:2]:
        copy.wait()
    start = start_ref[0]
    period = period_ref[0]

    row = lax.broadcasted_iota(jnp.int32, (n * SUB, 1), 0)
    late = row >= n * ITERS
    row = jnp.where(late, row - n * ITERS, row)
    block = row // ITERS - start
    block = jnp.where(block < 0, block + n, block)
    base = block * width
    item = row % ITERS
    ahead = base + jnp.minimum(period - base, width) + item
    ahead = jnp.where(ahead >= period, ahead - period, ahead)
    behind = base + item - ITERS
    behind = jnp.where(behind < 0, behind + period, behind)
    place = jnp.where(late, behind, ahead) + start * width
    place = jnp.where(place >= n * width, place - n * width, place)

    cpad[...] = jnp.zeros_like(cpad)

    def pick(j, total):
        at = pl.ds(pl.multiple_of(j * CHUNK, CHUNK), CHUNK)
        cpad[pl.ds(0, rs), :] = cs[:, at]
        cpad[pl.ds(rs, ri), :] = ci[:, at]
        column = lax.broadcasted_iota(jnp.int32, (n * SUB, CHUNK), 1) + j * CHUNK
        onehot = jnp.where(column == place, 1.0, 0.0).astype(jnp.bfloat16)
        rest = cpad[...]
        for _ in range(3):
            piece = rest.astype(jnp.bfloat16)
            rest = rest - piece.astype(jnp.float32)
            total = total + lax.dot_general(onehot, piece, NT, preferred_element_type=jnp.float32)
        return total

    picked = lax.fori_loop(
        0, cs.shape[1] // CHUNK, pick, jnp.zeros((n * SUB, LANES), jnp.float32)
    )
    packed = picked[:n * ITERS] + pltpu.roll(picked[n * ITERS:], half, 1)
    hsend[...] = packed.reshape(n, ITERS, LANES)
    recv_h[me] = hsend[me]

    pl.semaphore_wait(barrier, n - 1)
    for k in order:
        copies(1, k).start()
    for k in order:
        copies(2, k).start()
        copies(3, k).start()

    for copy in loads[2:5]:
        copy.wait()
    abt[...] = ab[...].T
    kt[...] = kkt[...].T
    link[pl.ds(0, SUB), :] = jnp.zeros((SUB, nx), jnp.float32)
    zn[pl.ds(rows, SUB), :] = jnp.zeros((SUB, nx), jnp.float32)

    mine = me - start
    mine = jnp.where(mine < 0, mine + n, mine)
    base = mine * width
    finish = jnp.minimum(period - base, width)

    for k in order:
        copies(1, k, True).wait_recv()

    lane = lax.broadcasted_iota(jnp.int32, (ITERS, LANES), 1)
    phase = (finish + 2 * width) % SUB
    for r, top in ((rs, 0), (ri, nx)):
        off = 0 if top == 0 else rs
        per = LANES // r
        for t in range(0, n * r, LANES):
            fore = jnp.zeros((ITERS, LANES), jnp.float32)
            aft = jnp.zeros((ITERS, LANES), jnp.float32)
            for q in range(min(per, n)):
                piece = recv_h[t // r + q]
                here = (lane >= q * r) & (lane < (q + 1) * r)
                fore = jnp.where(here, pltpu.roll(piece, (q * r - off) % LANES, 1), fore)
                aft = jnp.where(here, pltpu.roll(piece, (q * r - off - half) % LANES, 1), aft)
            at = pl.ds(top + t, LANES)
            hrow[pl.ds(0, ITERS), at] = -fore
            hrow[pl.ds(ITERS, ITERS), at] = -aft
    sub = lax.broadcasted_iota(jnp.int32, (SUB, 1), 0)
    negc[pl.ds(0, SUB), :] = jnp.where(sub >= ITERS, hrow[...], 0.0)
    for t in range(0, nw, LANES):
        at = pl.ds(t, LANES)
        ring = hrow[:, at]
        turned = ring
        for s in range(1, SUB):
            turned = jnp.where(phase == s, pltpu.roll(ring, s, 0), turned)
        hrow[:, at] = turned

    loads[5].wait()
    loads[6].wait()
    def arrived(kind, slot):
        src, dst = ((cs, recv_s), (ci, recv_i))[kind - 2]

        @pl.when(slot != me)
        def _():
            pltpu.make_async_remote_copy(
                src_ref=src.at[:, cols(slot)], dst_ref=dst.at[slot],
                send_sem=send_sem.at[kind, 0], recv_sem=recv_sem.at[kind, slot],
                device_id={"section": slot},
            ).wait_recv()

    def filled(r, value, at):
        ahead = sub + (r - SUB) - finish
        return jnp.where((ahead >= 0) & (ahead < ITERS), hrow[:, at], value)

    for kind, r, top, src in ((2, rs, 0, recv_s), (3, ri, nx, recv_i)):
        per = LANES // r
        for t in range(0, n * r, LANES):
            for q in range(per):
                arrived(kind, t // r + q)
            at = pl.ds(top + t, LANES)
            for b in range(0, width, LANES):
                stack = [src[t // r + q, :, pl.ds(b, LANES)] for q in range(per)]
                turned = jnp.concatenate(stack, axis=0).T
                for i in range(0, LANES, SUB):
                    down = SUB + b + i
                    negc[pl.ds(down, SUB), at] = filled(down, -turned[i:i + SUB], at)
            negc[pl.ds(SUB + width, SUB), at] = filled(
                SUB + width, jnp.zeros((SUB, LANES), jnp.float32), at
            )

    for it in range(ITERS):
        last = it == ITERS - 1
        if it == 0:
            for r in range(0, rows, ROWS):
                at = pl.ds(r, ROWS)
                rhs[at, :] = negc[at, :].astype(jnp.bfloat16)
        else:
            for t in range(0, nw, TILE):
                to = pl.ds(t, TILE)
                w[:, to] = dot(g[...], ab[:, to])
                known = c if t < nx else negc
                for r in range(0, rows, ROWS):
                    at = pl.ds(r, ROWS)
                    rhs[at, to] = (known[at, to] + scaled(w[at, to])).astype(jnp.bfloat16)
        for t in range(0, nw, TILE):
            to = pl.ds(t, TILE)
            w[:, to] = dot(rhs[...], kt[:, to])
            for r in range(0, rows, ROWS):
                at = pl.ds(r, ROWS)
                wb[at, to] = w[at, to].astype(jnp.bfloat16)
        if last:
            primal = jnp.zeros((SUB, LANES), jnp.float32)
            dual = jnp.zeros((SUB, LANES), jnp.float32)
        for t in range(0, nx, TILE):
            to = pl.ds(t, TILE)
            pred[:, to] = dot(wb[...], abt[:, to])
            for r in range(0, rows, ROWS):
                at = pl.ds(r, ROWS)
                q = pred[at, to]
                link[pl.ds(SUB + r, ROWS), to] = q + v[at, to] if it else q
            for r in range(0, rows, ROWS):
                at = pl.ds(r, ROWS)
                x = w[at, to]
                own = x + y[at, to] if it else x
                znew = 0.5 * (own + link[pl.ds(SUB + r - 1, ROWS), to])
                zn[at, to] = znew
                if not last:
                    ynew = own - znew
                    y[at, to] = ynew
                    c[at, to] = negc[at, to] + scaled(znew - ynew)
                    if it == ITERS - 2:
                        z[at, to] = znew
            if not last:
                for r in range(0, rows, ROWS):
                    at = pl.ds(r, ROWS)
                    znext = zn[pl.ds(r + 1, ROWS), to]
                    vnew = link[pl.ds(SUB + r, ROWS), to] - znext
                    v[at, to] = vnew
                    g[at, to] = (znext - vnew).astype(jnp.bfloat16)
            else:
                for r in range(SUB, SUB + width, SUB):
                    at = pl.ds(r, SUB)
                    active = sub + (base + r - SUB) < period
                    znew = zn[at, to]
                    znext = zn[pl.ds(r + 1, SUB), to]
                    miss = (w[at, to] - znew) ** 2 + (pred[at, to] - znext) ** 2
                    change = znew - z[at, to]
                    miss = jnp.where(active, miss, 0.0)
                    change = jnp.where(active, change * change, 0.0)
                    for b in range(0, TILE, LANES):
                        primal = primal + miss[:, b:b + LANES]
                        dual = dual + change[:, b:b + LANES]

    part[pl.ds(0, 1), :] = jnp.sum(primal, axis=0, keepdims=True)
    part[pl.ds(1, 1), :] = RHO * RHO * jnp.sum(dual, axis=0, keepdims=True)
    recv_p[me] = part[...]
    for k in order:
        copies(0, k).start()

    for b in range(0, width, LANES):
        to = pl.ds(b, LANES)
        lane = lax.broadcasted_iota(jnp.int32, (1, LANES), 1)
        active = lane + (base + b) < period
        for t in range(0, nw, LANES):
            value = jnp.where(active, w[pl.ds(SUB + b, LANES), pl.ds(t, LANES)].T, 0.0)
            if t < nx:
                xo[pl.ds(t, LANES), to] = value
                zo[pl.ds(t, LANES), to] = jnp.where(
                    active, zn[pl.ds(SUB + b, LANES), pl.ds(t, LANES)].T, 0.0
                )
            else:
                uo[pl.ds(t - nx, LANES), to] = value
    for k in order:
        copies(0, k, True).wait_recv()
    total = recv_p[0]
    for s in range(1, n):
        total = total + recv_p[s]
    total_out[...] = total
    for kind in range(4):
        for k in order:
            copies(kind, k).wait_send()


def store(x, u, z, total, x_out, u_out, z_out, norm_out, norm, sem):
    moves = [
        pltpu.make_async_copy(src, dst, sem.at[i])
        for i, (src, dst) in enumerate(((x, x_out), (u, u_out), (z, z_out)))
    ]
    for move in moves:
        move.start()
    both = jnp.sum(total[...], axis=1, keepdims=True)
    both = jnp.sqrt(jnp.broadcast_to(both, (2, LANES)))
    norm[0] = jnp.max(both[:1])
    norm[1] = jnp.max(both[1:])
    last = pltpu.make_async_copy(norm, norm_out, sem.at[3])
    last.start()
    for move in moves:
        move.wait()
    last.wait()


def local(a, b, kkt, lin_state, lin_input, block_start, period):
    n = lax.axis_size("section")
    width = lin_state.shape[1] // n
    rows = width + 2 * SUB
    nx, nu = b.shape
    nw = nx + nu
    rs, ri = lin_state.shape[0], lin_input.shape[0]
    f32, bf16 = jnp.float32, jnp.bfloat16
    anyspec = pl.BlockSpec(memory_space=pl.ANY)
    smem = pl.BlockSpec(memory_space=pltpu.SMEM)
    vspec = pl.BlockSpec(memory_space=pltpu.VMEM)
    hbm = pl.BlockSpec(memory_space=pltpu.HBM)
    vmem = pltpu.VMEM
    inputs = [
        pltpu.with_memory_space_constraint(value, pltpu.HBM)
        for value in (a, b, kkt, lin_state, lin_input)
    ]
    results = pl.pallas_call(
        functools.partial(kernel, n, width),
        name="admm",
        out_shape=(
            jax.ShapeDtypeStruct((nx, width), f32),
            jax.ShapeDtypeStruct((nu, width), f32),
            jax.ShapeDtypeStruct((nx, width), f32),
            jax.ShapeDtypeStruct((2, LANES), f32),
        ),
        in_specs=[hbm] * 5 + [smem] * 2,
        out_specs=(vspec,) * 4,
        scratch_shapes=[
            vmem((nx, nw), bf16), vmem((nw, nx), bf16), vmem((nw, nw), bf16), vmem((nw, nw), bf16),
            vmem(lin_state.shape, f32), vmem(lin_input.shape, f32),
            vmem((n, rs, width), f32), vmem((n, ri, width), f32),
            vmem((LANES, CHUNK), f32),
            vmem((n, ITERS, LANES), f32), vmem((n, ITERS, LANES), f32), vmem((SUB, nw), f32),
            vmem((rows, nw), f32), vmem((rows, nw), bf16), vmem((rows, nw), f32),
            vmem((rows, nw), bf16), vmem((rows, nx), f32),
            vmem((rows + SUB, nx), f32), vmem((rows + SUB, nx), f32),
            vmem((rows, nx), f32), vmem((rows, nx), f32), vmem((rows, nx), f32), vmem((rows, nx), f32),
            vmem((rows, nx), bf16),
            vmem((2, LANES), f32), vmem((n, 2, LANES), f32),
            pltpu.SemaphoreType.DMA((7,)),
            pltpu.SemaphoreType.DMA((4, n)), pltpu.SemaphoreType.DMA((4, n)),
        ],
        compiler_params=pltpu.CompilerParams(
            collective_id=0, has_side_effects=True, vmem_limit_bytes=24000000
        ),
    )(*inputs, block_start, period)
    return pl.pallas_call(
        store,
        name="store",
        out_shape=tuple(jax.ShapeDtypeStruct(r.shape, f32) for r in results[:3])
        + (jax.ShapeDtypeStruct((2,), f32),),
        in_specs=[anyspec] * 3 + [vspec],
        out_specs=(anyspec,) * 4,
        scratch_shapes=[pltpu.SMEM((2,), f32), pltpu.SemaphoreType.DMA((4,))],
        compiler_params=pltpu.CompilerParams(vmem_limit_bytes=4000000),
    )(*results)


def solution(mesh):
    return jax.shard_map(
        local,
        mesh=mesh,
        in_specs=(
            P("plant", None),
            P("plant", None),
            P("plant", None),
            P(("plant", "section"), None),
            P(("plant", "section"), None),
            P("plant"),
            P("plant"),
        ),
        out_specs=(P("plant", "section"), P("plant", "section"), P("plant", "section"), P("plant")),
        check_vma=False,
    )
```
